32 devices in a mesh: pb: 4 (over x, core), pq: 8 (over z, y).
Axes of the slice: x: 2, y: 2, z: 4, core: 2. Of those that a mesh axis runs over, the one named last changes fastest.
Arguments:
- chol_vv: bfloat16 [176, 1792, 1792], P('pb', 'pq'), may hold values from -6 to 6
- chol_ov: bfloat16 [176, 256, 1792], P('pb', 'pq'), may hold values from -6 to 6
- chol_oo: bfloat16 [176, 256, 256], P('pb', 'pq'), may hold values from -6 to 6
- chol_vo: bfloat16 [176, 256, 1792], P('pb', None, 'pq'), may hold values from -6 to 6
- amplitudes: bfloat16 [256, 1792], P(None, 'pq'), may hold values from -0.125 to 0.125
Outputs:
- dressed: bfloat16 [176, 256, 1792], P('pb', 'pq')
- fock_ov: float32 [256, 1792], P('pq')
The draws below stay inside these ranges and needn't reach their ends.
All inputs are finite; a program needn't handle non-finite values.
Results may differ from the reference program's by a relative error of at most 0.0081.
Values may be sent and summed in bfloat16 or wider, within the bound.
A program may use at most 128 MiB of HBM per device.

```python
import jax
import jax.numpy as jnp
from jax import lax

NOCC = 256
NVIRT = 1792
QB = 44
NQ = 176
N_PB = 4


def levels(rng, dims, cuts, low, top_value):
    loudness, own = 1.0, jax.random.fold_in(rng, 6)
    for dim, shards_of in cuts:
        heights = jnp.exp(jax.random.uniform(jax.random.fold_in(own, dim), (shards_of,), jnp.float32, low / len(cuts), top_value / len(cuts)))
        loudness = loudness * jnp.repeat(heights, dims[dim] // shards_of).reshape([-1 if axis == dim else 1 for axis in range(len(dims))])
    return loudness


def noise(own_key, dims, spread, bound, split=(), dtype=jnp.bfloat16):
    drawn = jax.random.normal(own_key, dims, jnp.float32) * spread
    if len(split) > 0:
        drawn = levels(own_key, dims, split, -0.22, 0.18) * drawn
    return jnp.clip(drawn, min=-bound, max=bound).astype(dtype)


def setup_inputs(seed: int = 0) -> dict:
    splits = jax.random.split(jax.random.key(seed), 6)
    chol_vv = noise(splits[0], (NQ, NVIRT, NVIRT), 1.0, 6.0, ((0, 4), (1, 8)))
    chol_ov = noise(splits[1], (NQ, NOCC, NVIRT), 1.0, 6.0, ((0, 4), (1, 8)))
    chol_oo = noise(splits[2], (NQ, NOCC, NOCC), 1.0, 6.0, ((0, 4), (1, 8)))
    chol_vo = noise(splits[3], (NQ, NOCC, NVIRT), 1.0, 6.0, ((0, 4), (2, 8)))
    amplitudes = noise(splits[4], (NOCC, NVIRT), NVIRT ** -0.5, 0.125, ((1, 8),))
    return {"chol_vv": chol_vv, "chol_ov": chol_ov, "chol_oo": chol_oo, "chol_vo": chol_vo, "amplitudes": amplitudes}


def reference(chol_vv, chol_ov, chol_oo, chol_vo, amplitudes):
    def one_vector(blocks):
        block_vv, block_ov, block_oo, block_vo = blocks
        lprime = (block_oo.astype(jnp.float32) + jnp.dot(block_ov, amplitudes.T, preferred_element_type=jnp.float32)).astype(jnp.bfloat16)
        direct = jnp.dot(amplitudes, block_vv.T, preferred_element_type=jnp.float32)
        occupied = jnp.dot(lprime.T, amplitudes, preferred_element_type=jnp.float32)
        return (block_vo.astype(jnp.float32) + direct - occupied).astype(jnp.bfloat16)

    dressed = lax.map(one_vector, (chol_vv, chol_ov, chol_oo, chol_vo))
    amps_wide = amplitudes.astype(jnp.float32)

    def one_coulomb(block):
        return 2.0 * jnp.sum(block.astype(jnp.float32) * amps_wide)

    coulomb = lax.map(one_coulomb, dressed)

    def add_vector(total, item):
        weight, block = item
        return total + weight * block.astype(jnp.float32), None

    start = jnp.zeros(amplitudes.shape, jnp.float32)
    total, unused = lax.scan(add_vector, start, (coulomb, dressed))
    fock_ov = total / (QB * N_PB)
    return dressed, fock_ov
```

```python
import functools

import jax
import jax.numpy as jnp
from jax import lax
from jax.experimental import pallas as pl
from jax.experimental.pallas import tpu as pltpu
from jax.sharding import PartitionSpec as P

MESH = pl.DeviceIdType.MESH


def per_device(chol_vv, chol_ov, chol_oo, chol_vo, amplitudes):
    batch = chol_vv.shape[0]
    occ_rows = chol_ov.shape[1]
    whole_amps = lax.all_gather(amplitudes, "pq", axis=1, tiled=True)
    lprime = (
        chol_oo.astype(jnp.float32)
        + jnp.einsum("qjb,ib->qji", chol_ov, whole_amps, preferred_element_type=jnp.float32)
    ).astype(jnp.bfloat16)
    direct = jnp.einsum("qab,ib->qia", chol_vv, whole_amps, preferred_element_type=jnp.float32)
    partial_sum = chol_vo.astype(jnp.float32) + direct
    occupied = jnp.einsum(
        "qji,ja->qia",
        lax.all_gather(lprime, "pq", axis=1, tiled=True),
        amplitudes,
        preferred_element_type=jnp.float32,
    )
    local_dressed = (partial_sum - occupied).astype(jnp.bfloat16)
    dressed = lax.all_to_all(local_dressed, "pq", split_axis=1, concat_axis=2, tiled=True)
    row_start = lax.axis_index("pq") * occ_rows
    own_amps = lax.dynamic_slice_in_dim(whole_amps, row_start, occ_rows, 0)
    local_coulomb = 2.0 * jnp.einsum(
        "qia,ia->q", dressed, own_amps, preferred_element_type=jnp.float32
    )
    coulomb = lax.psum(local_coulomb, "pq")
    local_fock = jnp.sum(coulomb[:, None, None] * dressed.astype(jnp.float32), axis=0)
    fock_ov = lax.psum(local_fock, "pb") / (batch * lax.axis_size("pb"))
    return (dressed, fock_ov)


def kernel(
    n, n_pb, group,
    vv_hbm, ov_hbm, oo_hbm, vo_hbm, amps_ref,
    out_hbm, fock_ref,
    vv_buf, ov_buf, oo_buf, vo_buf, amps_t, amps, tiled, gram,
    sent, got, dressed, coul_sent, coul_got, fock_sent, fock_got,
    load_sem, own_sem, gather_send, gather_recv, send_sem, recv_sem,
    coul_send, coul_recv, fock_send, fock_recv, out_sem,
):
    me = lax.axis_index("pq")
    mine = lax.axis_index("pb")
    batch, virt, whole_virt = vv_hbm.shape
    rows, occ = ov_hbm.shape[1], oo_hbm.shape[2]
    steps = batch // group
    wide, deep = group * virt, group * rows
    peers = [lax.rem(me + d, n) for d in range(1, n)]
    partners = [mine + 1 - 2 * lax.rem(mine, 2)] if n_pb >= 2 else []
    if n_pb >= 4:
        partners.append(lax.rem(mine + 2, 4))

    def loads(step, slot):
        part = pl.ds(step * group, group)
        pairs = ((vv_hbm, vv_buf), (ov_hbm, ov_buf), (oo_hbm, oo_buf), (vo_hbm, vo_buf))
        return [
            pltpu.make_async_copy(src.at[part], dst.at[slot], load_sem.at[slot, k])
            for k, (src, dst) in enumerate(pairs)
        ]

    for copy in loads(0, 0):
        copy.start()

    barrier = pltpu.get_barrier_semaphore()
    for peer in peers:
        pl.semaphore_signal(barrier, inc=1, device_id={"pq": peer}, device_id_type=MESH)
    for partner in partners:
        pl.semaphore_signal(barrier, inc=1, device_id={"pb": partner}, device_id_type=MESH)
    pl.semaphore_wait(barrier, len(peers) + len(partners))

    def remote(src, dst, send, recv, where):
        return pltpu.make_async_remote_copy(
            src_ref=src, dst_ref=dst, send_sem=send, recv_sem=recv,
            device_id=where, device_id_type=MESH,
        )

    own_block = pl.ds(pl.multiple_of(me * virt, 16), virt)
    gathers = [
        remote(amps_ref, amps_t.at[own_block], gather_send.at[d], gather_recv.at[d], {"pq": peer})
        for d, peer in enumerate(peers)
    ]
    for copy in gathers:
        copy.start()
    own = pltpu.make_async_copy(amps_ref, amps_t.at[own_block], own_sem)
    own.start()
    own.wait()
    for copy in gathers:
        copy.wait()

    for s in range(n):
        block = amps_t[s * virt:(s + 1) * virt, :]
        amps_t_f32 = block.astype(jnp.float32)
        tiled[:, s * virt:(s + 1) * virt] = amps_t_f32.T
    for s in range(n):
        part = tiled[s * rows:(s + 1) * rows, :].astype(jnp.bfloat16)
        for q in range(group):
            amps[s * deep + q * rows:s * deep + (q + 1) * rows, :] = part
    own_rows = amps[pl.ds(pl.multiple_of(me * deep, 128), rows), :]
    gram[...] = jnp.dot(own_rows, amps_t[...], preferred_element_type=jnp.float32)
    coul_sent[...] = jnp.zeros_like(coul_sent)

    def exchange(step, d):
        return remote(
            sent.at[step, pl.ds(pl.multiple_of(peers[d] * rows, 16), rows)],
            got.at[step, me],
            send_sem.at[step, d], recv_sem.at[step, d], {"pq": peers[d]},
        )

    def produce(step, carry):
        slot = lax.rem(step, 2)

        @pl.when(step + 1 < steps)
        def _():
            for copy in loads(step + 1, 1 - slot):
                copy.start()

        for copy in loads(step, slot):
            copy.wait()
        vv = vv_buf[slot].reshape(wide, whole_virt)
        direct = jnp.dot(vv, amps_t[...], preferred_element_type=jnp.float32)
        direct = direct + vo_buf[slot].reshape(wide, occ).astype(jnp.float32)
        sent[step, :, 0:wide] = direct.T.astype(jnp.bfloat16)
        ov = ov_buf[slot].reshape(deep, whole_virt)
        lprime = jnp.dot(ov, amps_t[...], preferred_element_type=jnp.float32)
        lprime = lprime + oo_buf[slot].reshape(deep, occ).astype(jnp.float32)
        sent[step, :, wide:wide + deep] = lprime.T.astype(jnp.bfloat16)
        own_amps = amps_ref[...].astype(jnp.float32)
        at_row = lax.broadcasted_iota(jnp.int32, coul_sent.shape, 0) == step
        lane = lax.broadcasted_iota(jnp.int32, coul_sent.shape, 1)
        held = coul_sent[...]
        for q in range(group):
            from_direct = direct[q * virt:(q + 1) * virt] * own_amps
            from_occ = lprime[q * rows:(q + 1) * rows] * gram[...]
            value = jnp.sum(from_direct) - jnp.sum(from_occ)
            held = jnp.where(at_row & (lane == q), value, held)
        coul_sent[...] = held
        got[step, me] = sent[step, pl.ds(pl.multiple_of(me * rows, 16), rows), :]
        for d in range(n - 1):
            exchange(step, d).start()
        return carry

    lax.fori_loop(0, steps, produce, 0)

    coulombs = [
        remote(coul_sent, coul_got.at[d], coul_send.at[d], coul_recv.at[d], {"pq": peer})
        for d, peer in enumerate(peers)
    ]
    for copy in coulombs:
        copy.start()

    def out_copy(step):
        part = pl.ds(step * group, group)
        return pltpu.make_async_copy(dressed.at[part], out_hbm.at[part], out_sem.at[step])

    def consume(step, carry):
        for d in range(n - 1):
            exchange(step, d).wait()
        lane_q = lax.broadcasted_iota(jnp.int32, (rows, deep), 1) // rows
        columns = []
        for s in range(n):
            piece = got[step, s, :, wide:wide + deep]
            columns.append(jnp.concatenate(
                [jnp.where(lane_q == q, piece, jnp.zeros_like(piece)) for q in range(group)], axis=0
            ))
        occupied = jnp.dot(
            jnp.concatenate(columns, axis=1), amps[...], preferred_element_type=jnp.float32
        )
        for q in range(group):
            partial_sum = jnp.concatenate(
                [got[step, s, :, q * virt:(q + 1) * virt].astype(jnp.float32) for s in range(n)],
                axis=1,
            )
            value = partial_sum - occupied[q * rows:(q + 1) * rows]
            dressed[step * group + q] = value.astype(jnp.bfloat16)
        out_copy(step).start()
        return carry

    lax.fori_loop(0, steps, consume, 0)

    for copy in coulombs:
        copy.wait()
    coulomb = coul_sent[...]
    for d in range(n - 1):
        coulomb = coulomb + coul_got[d]
    gram[0:coulomb.shape[0], 0:coulomb.shape[1]] = coulomb

    fock_ref[...] = jnp.zeros_like(fock_ref)

    def add_up(step, carry):
        lines = gram[0:coulomb.shape[0], 0:coulomb.shape[1]]
        at_row = lax.broadcasted_iota(jnp.int32, lines.shape, 0) == step
        lane = lax.broadcasted_iota(jnp.int32, lines.shape, 1)
        total = fock_ref[...]
        for q in range(group):
            weight = jnp.sum(jnp.where(at_row & (lane == q), lines, 0.0))
            total = total + weight * dressed[step * group + q].astype(jnp.float32)
        fock_ref[...] = total
        return carry

    lax.fori_loop(0, steps, add_up, 0)

    for k, partner in enumerate(partners):
        fock_sent[k] = fock_ref[...]
        copy = remote(
            fock_sent.at[k], fock_got.at[k], fock_send.at[k], fock_recv.at[k], {"pb": partner}
        )
        copy.start()
        copy.wait()
        fock_ref[...] = fock_sent[k] + fock_got[k]
    fock_ref[...] = fock_ref[...] * (2.0 / (batch * n_pb))

    def finish(step, carry):
        out_copy(step).wait()
        return carry

    lax.fori_loop(0, steps, finish, 0)


def fused(n, n_pb, group, chol_vv, chol_ov, chol_oo, chol_vo, amplitudes):
    batch, virt, whole_virt = chol_vv.shape
    rows, occ = chol_ov.shape[1], chol_oo.shape[2]
    steps = batch // group
    wide, deep = group * virt, group * rows
    lines = -(-steps // 8) * 8
    bf16, f32 = jnp.bfloat16, jnp.float32
    dma = pltpu.SemaphoreType.DMA
    hops = max(1, n_pb // 2)
    whole = pl.BlockSpec(memory_space=pltpu.VMEM)
    hbm = pl.BlockSpec(memory_space=pl.ANY)
    return pl.pallas_call(
        functools.partial(kernel, n, n_pb, group),
        out_shape=(
            jax.ShapeDtypeStruct((batch, rows, whole_virt), bf16),
            jax.ShapeDtypeStruct((rows, whole_virt), f32),
        ),
        in_specs=[hbm, hbm, hbm, hbm, whole],
        out_specs=(hbm, whole),
        scratch_shapes=[
            pltpu.VMEM((2, group, virt, whole_virt), bf16),
            pltpu.VMEM((2, group, rows, whole_virt), bf16),
            pltpu.VMEM((2, group, rows, occ), bf16),
            pltpu.VMEM((2, group, virt, occ), bf16),
            pltpu.VMEM((whole_virt, occ), bf16),
            pltpu.VMEM((n * deep, whole_virt), bf16),
            pltpu.VMEM((occ, whole_virt), f32),
            pltpu.VMEM((rows, occ), f32),
            pltpu.VMEM((steps, occ, wide + deep), bf16),
            pltpu.VMEM((steps, n, rows, wide + deep), bf16),
            pltpu.VMEM((batch, rows, whole_virt), bf16),
            pltpu.VMEM((lines, 128), f32),
            pltpu.VMEM((n - 1, lines, 128), f32),
            pltpu.VMEM((hops, rows, whole_virt), f32),
            pltpu.VMEM((hops, rows, whole_virt), f32),
            dma((2, 4)), dma, dma((n - 1,)), dma((n - 1,)),
            dma((steps, n - 1)), dma((steps, n - 1)),
            dma((n - 1,)), dma((n - 1,)), dma((hops,)), dma((hops,)), dma((steps,)),
        ],
        compiler_params=pltpu.CompilerParams(
            collective_id=0, has_side_effects=True, vmem_limit_bytes=60 * 1024 * 1024
        ),
    )(chol_vv, chol_ov, chol_oo, jnp.swapaxes(chol_vo, 1, 2), amplitudes.T)


def group_size(batch, virt, rows):
    for group in range(1, batch + 1):
        if batch % group == 0 and group * virt % 128 == 0 and group * rows % 128 == 0:
            return group
    return None


def solution(mesh):
    n, n_pb = mesh.shape["pq"], mesh.shape["pb"]
    in_specs = (
        P("pb", "pq", None),
        P("pb", "pq", None),
        P("pb", "pq", None),
        P("pb", None, "pq"),
        P(None, "pq"),
    )
    out_specs = (P("pb", "pq", None), P("pq", None))

    def body(chol_vv, chol_ov, chol_oo, chol_vo, amplitudes):
        batch, virt, unused = chol_vv.shape
        rows, occ = chol_ov.shape[1], chol_oo.shape[2]
        group = group_size(batch, virt, rows)
        fits = group is not None and group <= 8 and virt % 16 == 0 and rows % 16 == 0
        fits = fits and occ % 128 == 0 and n_pb in (1, 2, 4) and n > 1 and batch // group <= rows
        if fits:
            return fused(n, n_pb, group, chol_vv, chol_ov, chol_oo, chol_vo, amplitudes)
        return per_device(chol_vv, chol_ov, chol_oo, chol_vo, amplitudes)

    return jax.shard_map(
        body, mesh=mesh, in_specs=in_specs, out_specs=out_specs, check_vma=False
    )
```

```python
import functools

import jax
import jax.numpy as jnp
from jax import lax
from jax.experimental import pallas as pl
from jax.experimental.pallas import tpu as pltpu
from jax.sharding import PartitionSpec as P

MESH = pl.DeviceIdType.MESH


def per_device(chol_vv, chol_ov, chol_oo, chol_vo, amplitudes):
    batch = chol_vv.shape[0]
    occ_rows = chol_ov.shape[1]
    whole_amps = lax.all_gather(amplitudes, "pq", axis=1, tiled=True)
    lprime = (
        chol_oo.astype(jnp.float32)
        + jnp.einsum("qjb,ib->qji", chol_ov, whole_amps, preferred_element_type=jnp.float32)
    ).astype(jnp.bfloat16)
    direct = jnp.einsum("qab,ib->qia", chol_vv, whole_amps, preferred_element_type=jnp.float32)
    partial_sum = chol_vo.astype(jnp.float32) + direct
    occupied = jnp.einsum(
        "qji,ja->qia",
        lax.all_gather(lprime, "pq", axis=1, tiled=True),
        amplitudes,
        preferred_element_type=jnp.float32,
    )
    local_dressed = (partial_sum - occupied).astype(jnp.bfloat16)
    dressed = lax.all_to_all(local_dressed, "pq", split_axis=1, concat_axis=2, tiled=True)
    row_start = lax.axis_index("pq") * occ_rows
    own_amps = lax.dynamic_slice_in_dim(whole_amps, row_start, occ_rows, 0)
    local_coulomb = 2.0 * jnp.einsum(
        "qia,ia->q", dressed, own_amps, preferred_element_type=jnp.float32
    )
    coulomb = lax.psum(local_coulomb, "pq")
    local_fock = jnp.sum(coulomb[:, None, None] * dressed.astype(jnp.float32), axis=0)
    fock_ov = lax.psum(local_fock, "pb") / (batch * lax.axis_size("pb"))
    return (dressed, fock_ov)


def kernel(
    n, n_pb, group,
    vv_hbm, ov_hbm, oo_hbm, vo_hbm, amps_ref,
    dressed, fock_ref,
    vv_buf, ov_buf, oo_buf, vo_buf, amps_t, amps, tiled, gram,
    sent, got, coul_sent, coul_got, fock_sent, fock_got,
    load_sem, own_sem, gather_send, gather_recv, send_sem, recv_sem,
    coul_send, coul_recv, fock_send, fock_recv,
):
    me = lax.axis_index("pq")
    mine = lax.axis_index("pb")
    batch, virt, whole_virt = vv_hbm.shape
    rows, occ = ov_hbm.shape[1], oo_hbm.shape[2]
    steps = batch // group
    wide, deep = group * virt, group * rows
    peers = [lax.rem(me + d, n) for d in range(1, n)]
    core, place = lax.rem(mine, 2), mine // 2
    mate, across = mine + 1 - 2 * core, lax.rem(mine + 2, 4)
    partners = [mate, across]

    def loads(step, slot):
        part = pl.ds(step * group, group)
        pairs = ((vv_hbm, vv_buf), (ov_hbm, ov_buf), (oo_hbm, oo_buf), (vo_hbm, vo_buf))
        return [
            pltpu.make_async_copy(src.at[part], dst.at[slot], load_sem.at[slot, k])
            for k, (src, dst) in enumerate(pairs)
        ]

    for copy in loads(0, 0):
        copy.start()

    barrier = pltpu.get_barrier_semaphore()
    for peer in peers:
        pl.semaphore_signal(barrier, inc=1, device_id={"pq": peer}, device_id_type=MESH)
    for partner in partners:
        pl.semaphore_signal(barrier, inc=1, device_id={"pb": partner}, device_id_type=MESH)
    pl.semaphore_wait(barrier, len(peers) + len(partners))

    def remote(src, dst, send, recv, where):
        return pltpu.make_async_remote_copy(
            src_ref=src, dst_ref=dst, send_sem=send, recv_sem=recv,
            device_id=where, device_id_type=MESH,
        )

    half_virt, half_occ = virt // 2, occ // 2
    own_columns = pl.ds(pl.multiple_of(core * half_occ, 128), half_occ)

    def quarter(owner):
        first = pl.multiple_of(owner * virt + place * half_virt, 16)
        return amps_t.at[pl.ds(first, half_virt), own_columns]

    own_quarter = amps_ref.at[pl.ds(pl.multiple_of(place * half_virt, 16), half_virt), own_columns]
    gathers = [
        remote(own_quarter, quarter(me), gather_send.at[0, d], gather_recv.at[0, d], {"pq": peer})
        for d, peer in enumerate(peers)
    ]
    for copy in gathers:
        copy.start()
    own_block = pl.ds(pl.multiple_of(me * virt, 16), virt)
    own = pltpu.make_async_copy(amps_ref, amps_t.at[own_block], own_sem)
    own.start()
    own.wait()
    owners = [lax.rem(me + n - 1 - d, n) for d in range(n - 1)]
    crossing = [
        remote(quarter(owner), quarter(owner), gather_send.at[1, d], gather_recv.at[1, d], {"pb": across})
        for d, owner in enumerate(owners)
    ]
    swaps = []
    for d, owner in enumerate(owners):
        block = pl.ds(pl.multiple_of(owner * virt, 16), virt)
        half = amps_t.at[block, own_columns]
        swaps.append(remote(half, half, gather_send.at[2, d], gather_recv.at[2, d], {"pb": mate}))
    for d in range(n - 1):
        gathers[d].wait_recv()
        crossing[d].start()
    for d in range(n - 1):
        crossing[d].wait_recv()
        swaps[d].start()
    for d in range(n - 1):
        swaps[d].wait_recv()
    for copy in gathers + crossing + swaps:
        copy.wait_send()

    for s in range(n):
        block = amps_t[s * virt:(s + 1) * virt, :]
        amps_t_f32 = block.astype(jnp.float32)
        tiled[:, s * virt:(s + 1) * virt] = amps_t_f32.T
    for s in range(n):
        part = tiled[s * rows:(s + 1) * rows, :].astype(jnp.bfloat16)
        for q in range(group):
            amps[s * deep + q * rows:s * deep + (q + 1) * rows, :] = part
    own_rows = amps[pl.ds(pl.multiple_of(me * deep, 128), rows), :]
    gram[...] = jnp.dot(own_rows, amps_t[...], preferred_element_type=jnp.float32)
    coul_sent[...] = jnp.zeros_like(coul_sent)

    def exchange(step, d):
        return remote(
            sent.at[step, pl.ds(pl.multiple_of(peers[d] * rows, 16), rows)],
            got.at[step, me],
            send_sem.at[step, d], recv_sem.at[step, d], {"pq": peers[d]},
        )

    early = min(steps, 5)

    def produce(step, carry):
        slot = lax.rem(step, 2)

        @pl.when(step + 1 < steps)
        def _():
            for copy in loads(step + 1, 1 - slot):
                copy.start()

        for copy in loads(step, slot):
            copy.wait()
        vv = vv_buf[slot].reshape(wide, whole_virt)
        direct = jnp.dot(vv, amps_t[...], preferred_element_type=jnp.float32)
        direct = direct + vo_buf[slot].reshape(wide, occ).astype(jnp.float32)
        sent[step, :, 0:wide] = direct.T.astype(jnp.bfloat16)
        ov = ov_buf[slot].reshape(deep, whole_virt)
        lprime = jnp.dot(ov, amps_t[...], preferred_element_type=jnp.float32)
        lprime = lprime + oo_buf[slot].reshape(deep, occ).astype(jnp.float32)
        sent[step, :, wide:wide + deep] = lprime.T.astype(jnp.bfloat16)
        own_amps = amps_ref[...].astype(jnp.float32)
        at_row = lax.broadcasted_iota(jnp.int32, coul_sent.shape, 0) == step
        lane = lax.broadcasted_iota(jnp.int32, coul_sent.shape, 1)
        held = coul_sent[...]
        for q in range(group):
            from_direct = direct[q * virt:(q + 1) * virt] * own_amps
            from_occ = lprime[q * rows:(q + 1) * rows] * gram[...]
            value = jnp.sum(from_direct) - jnp.sum(from_occ)
            held = jnp.where(at_row & (lane == q), value, held)
        coul_sent[...] = held
        got[step, me] = sent[step, pl.ds(pl.multiple_of(me * rows, 16), rows), :]

        @pl.when(step < early)
        def _():
            for d in range(n - 1):
                exchange(step, d).start()

        return carry

    lax.fori_loop(0, steps, produce, 0)

    coulombs = [
        remote(coul_sent, coul_got.at[d], coul_send.at[d], coul_recv.at[d], {"pq": peer})
        for d, peer in enumerate(peers)
    ]
    for copy in coulombs:
        copy.start()

    def send(step, carry):
        for d in range(n - 1):
            exchange(step, d).start()
        return carry

    lax.fori_loop(early, steps, send, 0)

    for copy in coulombs:
        copy.wait()
    coulomb = coul_sent[...]
    for d in range(n - 1):
        coulomb = coulomb + coul_got[d]
    coul_sent[...] = coulomb
    fock_ref[...] = jnp.zeros_like(fock_ref)

    def consume(step, carry):
        for d in range(n - 1):
            exchange(step, d).wait()
        lane_q = lax.broadcasted_iota(jnp.int32, (rows, deep), 1) // rows
        columns = []
        for s in range(n):
            piece = got[step, s, :, wide:wide + deep]
            columns.append(jnp.concatenate(
                [jnp.where(lane_q == q, piece, jnp.zeros_like(piece)) for q in range(group)], axis=0
            ))
        occupied = jnp.dot(
            jnp.concatenate(columns, axis=1), amps[...], preferred_element_type=jnp.float32
        )
        weights = coul_sent[...]
        at_row = lax.broadcasted_iota(jnp.int32, weights.shape, 0) == step
        lane = lax.broadcasted_iota(jnp.int32, weights.shape, 1)
        total = fock_ref[...]
        for q in range(group):
            partial_sum = jnp.concatenate(
                [got[step, s, :, q * virt:(q + 1) * virt].astype(jnp.float32) for s in range(n)],
                axis=1,
            )
            value = (partial_sum - occupied[q * rows:(q + 1) * rows]).astype(jnp.bfloat16)
            dressed[step * group + q] = value
            weight = jnp.sum(jnp.where(at_row & (lane == q), weights, 0.0))
            total = total + weight * value.astype(jnp.float32)
        fock_ref[...] = total
        return carry

    lax.fori_loop(0, steps, consume, 0)

    half_rows = rows // 2
    own_half = pl.ds(pl.multiple_of(core * half_rows, 8), half_rows)
    mate_half = pl.ds(pl.multiple_of((1 - core) * half_rows, 8), half_rows)

    def swap(k, value, partner):
        fock_sent[k] = value
        copy = remote(
            fock_sent.at[k], fock_got.at[k], fock_send.at[k], fock_recv.at[k], {"pb": partner}
        )
        copy.start()
        copy.wait()
        return fock_got[k]

    both = swap(0, fock_ref[mate_half, :], mate) + fock_ref[own_half, :]
    every = (swap(1, both, across) + both) * (2.0 / (batch * n_pb))
    fock_ref[own_half, :] = every
    fock_ref[mate_half, :] = swap(2, every, mate)


def fused(n, n_pb, group, chol_vv, chol_ov, chol_oo, chol_vo, amplitudes):
    batch, virt, whole_virt = chol_vv.shape
    rows, occ = chol_ov.shape[1], chol_oo.shape[2]
    steps = batch // group
    wide, deep = group * virt, group * rows
    lines = -(-steps // 8) * 8
    bf16, f32 = jnp.bfloat16, jnp.float32
    dma = pltpu.SemaphoreType.DMA
    hops = 3
    whole = pl.BlockSpec(memory_space=pltpu.VMEM)
    hbm = pl.BlockSpec(memory_space=pl.ANY)
    return pl.pallas_call(
        functools.partial(kernel, n, n_pb, group),
        out_shape=(
            pltpu.VMEM((batch, rows, whole_virt), bf16),
            jax.ShapeDtypeStruct((rows, whole_virt), f32),
        ),
        in_specs=[hbm, hbm, hbm, hbm, whole],
        out_specs=(whole, whole),
        scratch_shapes=[
            pltpu.VMEM((2, group, virt, whole_virt), bf16),
            pltpu.VMEM((2, group, rows, whole_virt), bf16),
            pltpu.VMEM((2, group, rows, occ), bf16),
            pltpu.VMEM((2, group, virt, occ), bf16),
            pltpu.VMEM((whole_virt, occ), bf16),
            pltpu.VMEM((n * deep, whole_virt), bf16),
            pltpu.VMEM((occ, whole_virt), f32),
            pltpu.VMEM((rows, occ), f32),
            pltpu.VMEM((steps, occ, wide + deep), bf16),
            pltpu.VMEM((steps, n, rows, wide + deep), bf16),
            pltpu.VMEM((lines, 128), f32),
            pltpu.VMEM((n - 1, lines, 128), f32),
            pltpu.VMEM((hops, rows // 2, whole_virt), f32),
            pltpu.VMEM((hops, rows // 2, whole_virt), f32),
            dma((2, 4)), dma, dma((3, n - 1)), dma((3, n - 1)),
            dma((steps, n - 1)), dma((steps, n - 1)),
            dma((n - 1,)), dma((n - 1,)), dma((hops,)), dma((hops,)),
        ],
        compiler_params=pltpu.CompilerParams(
            collective_id=0, has_side_effects=True, vmem_limit_bytes=44 * 1024 * 1024
        ),
    )(chol_vv, chol_ov, chol_oo, jnp.swapaxes(chol_vo, 1, 2), amplitudes.T)


def group_size(batch, virt, rows):
    for group in range(1, batch + 1):
        if batch % group == 0 and group * virt % 128 == 0 and group * rows % 128 == 0:
            return group
    return None


def solution(mesh):
    n, n_pb = mesh.shape["pq"], mesh.shape["pb"]
    in_specs = (
        P("pb", "pq", None),
        P("pb", "pq", None),
        P("pb", "pq", None),
        P("pb", None, "pq"),
        P(None, "pq"),
    )
    out_specs = (P("pb", "pq", None), P("pq", None))

    def body(chol_vv, chol_ov, chol_oo, chol_vo, amplitudes):
        batch, virt, unused = chol_vv.shape
        rows, occ = chol_ov.shape[1], chol_oo.shape[2]
        group = group_size(batch, virt, rows)
        fits = group is not None and group <= 8 and virt % 32 == 0 and rows % 16 == 0
        fits = fits and occ % 256 == 0 and n_pb == 4 and n > 1 and batch // group <= rows
        if fits:
            return fused(n, n_pb, group, chol_vv, chol_ov, chol_oo, chol_vo, amplitudes)
        return per_device(chol_vv, chol_ov, chol_oo, chol_vo, amplitudes)

    return jax.shard_map(
        body, mesh=mesh, in_specs=in_specs, out_specs=out_specs, check_vma=False
    )
```
